128 devices in a mesh: ctx: 16 (over y, x), tp: 8 (over z, core).
Axes of the slice: x: 4, y: 4, z: 4, core: 2. Of those that a mesh axis runs over, the one named last changes fastest.
Arguments:
- hidden: bfloat16 [8, 8192], P(None, 'ctx'), may hold values from -4.8 to 4.8, as said below
- norm_gains: bfloat16 [4, 8192], P(None, 'ctx'), may hold values from 0.5 to 1.5
- w_query: bfloat16 [4, 8192, 8192], P(None, 'ctx', 'tp'), may hold values from -0.0625 to 0.0625
- w_key: bfloat16 [4, 8192, 1024], P(None, 'ctx', 'tp'), may hold values from -0.125 to 0.125
- w_value: bfloat16 [4, 8192, 1024], P(None, 'ctx', 'tp'), may hold values from -0.125 to 0.125
- w_out: bfloat16 [4, 8192, 8192], P(None, 'tp', 'ctx'), may hold values from -0.0625 to 0.0625
- key_cache: bfloat16 [4, 8, 8, 2048, 128], P(None, None, 'tp', 'ctx'), may hold values from -9 to 9
- value_cache: bfloat16 [4, 8, 8, 2048, 128], P(None, None, 'tp', 'ctx'), may hold values from -6 to 6
- lengths: int32 [8], replicated, may hold values from 1 to 2048, 8200 in all
Outputs:
- updated: float32 [8, 8192], P(None, 'ctx')
The draws below stay inside these ranges and needn't reach their ends.
Inputs may be any that keep to these rules, and one draw needn't show every extreme that they name: Each sequence has lengths[b] valid cache positions 0 .. lengths[b] - 1, between 1 and 2048; the longest sequence has exactly 2048; the new token sits at position lengths[b]. `hidden`: activations of order 0.2; in each block of 512 consecutive features one sequence, chosen at random, has entries four times larger.
All inputs are finite; a program needn't handle non-finite values.
Results may differ from the reference program's by a relative error of at most 0.02.
Values sent between devices are 32-bit elements.
A program may use at most 64 MiB of HBM per device.

```python
import math
import jax
import jax.numpy as jnp
import numpy as np
from jax import lax

D = 8192
HQ = 64
KVH = 8
HD = 128
LAYERS = 4
BATCH = 8
CAP = 2048
D_DEV = 512


def draw_hidden(key, part):
    base_key, owner_key = jax.random.split(jax.random.fold_in(key, 7))
    block_count = D // D_DEV
    owners = jax.random.randint(owner_key, (block_count,), 0, BATCH)
    column_owner = owners[jnp.arange(D) // D_DEV]
    factor = jnp.where(column_owner[None, :] == jnp.arange(BATCH)[:, None], 4.0, 1.0)
    base_draw = jnp.clip(jax.random.normal(base_key, (BATCH, D), jnp.float32), -6.0, 6.0)
    return (0.2 * factor * base_draw).astype(jnp.bfloat16)


def block_scale(rng, extent, pieces, smallest, high):
    gain = 1.0
    for axis_at, parts in pieces:
        draws = jax.random.uniform(jax.random.fold_in(jax.random.fold_in(rng, 6), axis_at), (parts,), jnp.float32, smallest / len(pieces), high / len(pieces))
        gain = gain * jnp.repeat(jnp.exp(draws), extent[axis_at] // parts).reshape((-1,) + (1,) * (len(extent) - 1 - axis_at))
    return gain


def profile(count, total, reach, slope):
    portions = [(1 << 20) // math.isqrt(grade ** slope) + 1 for grade in range(2, count + 1)]
    surplus, given = total - reach - (count - 1), [1] * (count - 1)
    while surplus > 0:
        movable = [i for i in range(count - 1) if given[i] < reach]
        mass, remaining = sum([portions[i] for i in movable]), surplus
        for i in movable:
            extra = min(reach - given[i], max(1, remaining * portions[i] // mass), surplus)
            given[i] = given[i] + extra
            surplus = surplus - extra
    return np.array([reach] + given)


def ragged(rng, amount, total, most, lean):
    if amount == 2:
        one = jax.random.randint(rng, (), max(1, total - most), min(most, total - 1) + 1)
        return jnp.stack([one, total - one])
    sizes = jnp.asarray(profile(amount, total, most, lean), jnp.int32)
    couples = (amount - 1) // 2
    source_of, taker = sizes[1:1 + 2 * couples:2], sizes[2:2 + 2 * couples:2]
    slack = jnp.minimum(source_of - 1, most - taker)
    shifted = jax.random.randint(jax.random.fold_in(rng, 1), (couples,), 0, 1 << 20) % (slack + 1)
    sizes = sizes.at[1:1 + 2 * couples:2].set(source_of - shifted).at[2:2 + 2 * couples:2].set(taker + shifted)
    return sizes[jax.random.permutation(jax.random.fold_in(rng, 2), amount)]


def scatter_about(stream_key, dims, scale, limit, pieces=(), kind=jnp.bfloat16):
    array = scale * jax.random.normal(stream_key, dims, jnp.float32)
    if pieces:
        array = array * block_scale(stream_key, dims, pieces, -0.22, 0.18)
    return jnp.clip(array, -limit, limit).astype(kind)


def setup_inputs(seed: int = 0) -> dict:
    key_list = jax.random.split(jax.random.key(seed), 10)
    hidden = draw_hidden(jax.random.fold_in(key_list[9], 71), 0)
    norm_gains = jnp.clip(1.0 + 0.1 * jax.random.normal(key_list[1], (LAYERS, D), jnp.float32), 0.5, 1.5).astype(jnp.bfloat16)
    w_query = scatter_about(key_list[2], (LAYERS, D, HQ * HD), D ** -0.5, 0.0625, ((1, 16), (2, 8)))
    w_key = scatter_about(key_list[3], (LAYERS, D, KVH * HD), (D // 4) ** -0.5, 0.125, ((1, 16), (2, 8)))
    w_value = scatter_about(key_list[4], (LAYERS, D, KVH * HD), (D // 4) ** -0.5, 0.125, ((1, 16), (2, 8)))
    w_out = scatter_about(key_list[5], (LAYERS, HQ * HD, D), (HQ * HD) ** -0.5, 0.0625, ((1, 8), (2, 16)))
    key_cache = scatter_about(key_list[6], (LAYERS, BATCH, KVH, CAP, HD), 1.5, 9.0, ((2, 8), (3, 16)))
    value_cache = scatter_about(key_list[7], (LAYERS, BATCH, KVH, CAP, HD), 1.0, 6.0, ((2, 8), (3, 16)))
    lengths = ragged(key_list[8], BATCH, BATCH * CAP // 2 + BATCH, CAP, 2).astype(jnp.int32)
    return dict(hidden=hidden, norm_gains=norm_gains, w_query=w_query, w_key=w_key, w_value=w_value, w_out=w_out, key_cache=key_cache, value_cache=value_cache, lengths=lengths)


mask_fill = -1e+30
norm_eps = 1e-05
rope_base = 500000.0

def rotate(vectors, positions):
    width = vectors.shape[-1]
    half_width = width // 2
    exponents = jnp.arange(half_width, dtype=jnp.float32) * (2.0 / width)
    frequency = jnp.exp(-exponents * math.log(rope_base))
    angles = positions.astype(jnp.float32)[:, None] * frequency[None, :]
    cosine = jnp.cos(angles)[:, None, :]
    sine_part = jnp.sin(angles)[:, None, :]
    first_half = vectors[..., :half_width]
    second_half = vectors[..., half_width:]
    return jnp.concatenate([first_half * cosine - second_half * sine_part, second_half * cosine + first_half * sine_part], axis=-1)

def reference(hidden, norm_gains, w_query, w_key, w_value, w_out, key_cache, value_cache, lengths):
    stream = hidden.astype(jnp.float32)
    group_size = HQ // KVH
    logit_multiplier = 1.0 / math.sqrt(HD)
    positions = jnp.arange(CAP, dtype=jnp.int32)
    usable = (positions[None, :] < lengths[:, None])[:, None, None, :]
    for layer_idx in range(LAYERS):
        reciprocal_value = lax.rsqrt(lax.optimization_barrier(jnp.sum(stream * stream, axis=1)) / D + norm_eps)
        scaled = (stream * norm_gains[layer_idx].astype(jnp.float32)).astype(jnp.bfloat16)
        raw_query = jnp.dot(scaled, w_query[layer_idx], preferred_element_type=jnp.float32)
        raw_key = jnp.dot(scaled, w_key[layer_idx], preferred_element_type=jnp.float32)
        raw_value = jnp.dot(scaled, w_value[layer_idx], preferred_element_type=jnp.float32)
        query = rotate((raw_query * reciprocal_value[:, None]).reshape(BATCH, HQ, HD), lengths).astype(jnp.bfloat16)
        fresh_lookup_vector = rotate((raw_key * reciprocal_value[:, None]).reshape(BATCH, KVH, HD), lengths).astype(jnp.bfloat16)
        new_value = (raw_value * reciprocal_value[:, None]).reshape(BATCH, KVH, HD).astype(jnp.bfloat16)
        shared_head_sets = query.reshape(BATCH, KVH, group_size, HD).astype(jnp.float32)
        scores = jnp.einsum('bkgd,bksd->bkgs', shared_head_sets, key_cache[layer_idx].astype(jnp.float32), precision=lax.Precision.HIGHEST) * logit_multiplier
        self_match_logit = jnp.einsum('uryj,urj->ury', shared_head_sets, fresh_lookup_vector.astype(jnp.float32), precision=lax.Precision.HIGHEST) * logit_multiplier
        masked = jnp.where(usable, scores, mask_fill)
        largest = jnp.maximum(lax.optimization_barrier(jnp.max(masked, axis=-1)), self_match_logit)
        attention_probabilities = jnp.where(usable, jnp.exp(masked - largest[..., None]), 0.0)
        fresh = jnp.exp(self_match_logit - largest)
        nearest_whole = lax.optimization_barrier(attention_probabilities.astype(jnp.bfloat16)).astype(jnp.float32)
        fresh_rounded = lax.optimization_barrier(fresh.astype(jnp.bfloat16)).astype(jnp.float32)
        numerator = jnp.einsum('bkgs,bksd->bkgd', nearest_whole, value_cache[layer_idx].astype(jnp.float32), precision=lax.Precision.HIGHEST)
        numerator = numerator + fresh_rounded[..., None] * new_value.astype(jnp.float32)[:, :, None, :]
        denominator = lax.optimization_barrier(jnp.sum(attention_probabilities, axis=-1)) + fresh
        context = (numerator / denominator[..., None]).reshape(BATCH, HQ * HD).astype(jnp.bfloat16)
        stream = stream + jnp.dot(context, w_out[layer_idx], preferred_element_type=jnp.float32)
    return stream
```

```python
import functools
import math

import jax
import jax.numpy as jnp
from jax import lax
from jax.experimental import pallas as pl
from jax.experimental.pallas import tpu as pltpu
from jax.sharding import PartitionSpec as P

D = 8192
LAYERS = 4
BATCH = 8
HEADS = 8
HD = 128
FEATS = 512
POS = 128
NX = 4
NTP = 8
mask_fill = -1e30
norm_eps = 1e-05
rope_base = 500000.0
logit_multiplier = 1.0 / math.sqrt(HD)
T0, T1 = 6, 5
TB = 5


def kernel(
    hidden, gains, wq, wk, wv, wo, kc, vc, lengths,
    out,
    hid_s, gain_s, len_s, wq_s, wk_s, wv_s, wo_s, kc_s, vc_s,
    a0, a1, b0, b1, cbuf,
    load_sem, w_sem, a_send, a_recv, b_send, b_recv, c_send, c_recv,
):
    ctx = lax.axis_index("ctx")
    tp = lax.axis_index("tp")
    y = ctx // NX
    x = ctx % NX

    loads = [
        pltpu.make_async_copy(hidden, hid_s, load_sem.at[0]),
        pltpu.make_async_copy(gains, gain_s, load_sem.at[1]),
        pltpu.make_async_copy(lengths, len_s, load_sem.at[2]),
    ]
    for c in loads:
        c.start()
    weights = []
    for l in range(LAYERS):
        row = [
            pltpu.make_async_copy(src.at[l], dst.at[l], w_sem.at[l, i])
            for i, (src, dst) in enumerate(
                ((wq, wq_s), (wk, wk_s), (wv, wv_s), (kc, kc_s), (vc, vc_s), (wo, wo_s))
            )
        ]
        weights.append(row)
        for c in row:
            c.start()

    def along(axis, k):
        if axis == "x":
            return {"ctx": y * NX + (x + k) % NX}
        return {"ctx": ((y + k) % NX) * NX + x}

    barrier = pltpu.get_barrier_semaphore()
    for axis in ("x", "y"):
        for k in (2, 1, 3):
            pl.semaphore_signal(barrier, inc=1, device_id=along(axis, k))
    for k in range(1, NTP):
        pl.semaphore_signal(barrier, inc=1, device_id={"tp": (tp + k) % NTP})

    pending = []

    def exchange(buf, l, stage, axis, send, recv):
        copies = []
        for k in (2, 1, 3):
            c = pltpu.make_async_remote_copy(
                src_ref=buf.at[l, stage, 0],
                dst_ref=buf.at[l, stage, k],
                send_sem=send.at[l, stage, k],
                recv_sem=recv.at[l, stage, k],
                device_id=along(axis, k),
            )
            c.start()
            copies.append(c)
        pending.extend(copies)
        return copies

    def arrive(copies):
        for c in copies:
            c.wait_recv()

    for c in loads:
        c.wait()

    lane = lax.broadcasted_iota(jnp.int32, (BATCH, HD), 1)
    sub = lax.broadcasted_iota(jnp.int32, (BATCH, HD), 0)
    lens = jnp.full((BATCH, HD), len_s[0], jnp.int32)
    for b in range(1, BATCH):
        lens = jnp.where(sub == b, len_s[b], lens)
    exponents = (lane % (HD // 2)).astype(jnp.float32) * (2.0 / HD)
    angles = lens.astype(jnp.float32) * jnp.exp(-exponents * math.log(rope_base))
    cosine = jnp.cos(angles)
    sine = jnp.sin(angles)
    sine = jnp.where(lane < HD // 2, -sine, sine)
    usable = (ctx * POS + lane) < lens
    usable = jnp.concatenate([usable.astype(jnp.int32)] * HEADS, axis=0) > 0
    row_seq = lax.broadcasted_iota(jnp.int32, (HEADS * BATCH, HD), 0) % BATCH

    def tile(buf, l, stage, slot, t):
        return buf[l, stage, slot, pl.ds(t * 8, 8), :]

    def put(buf, l, stage, slot, t, value):
        buf[l, stage, slot, pl.ds(t * 8, 8), :] = value

    def summed(buf, l, stage, t):
        return (tile(buf, l, stage, 0, t) + tile(buf, l, stage, 1, t)) + (
            tile(buf, l, stage, 2, t) + tile(buf, l, stage, 3, t)
        )

    def spread(compact, j):
        return jnp.broadcast_to(compact[:, j : j + 1], (BATCH, HD))

    stream = hid_s[...].astype(jnp.float32)
    for l in range(LAYERS):
        squares = stream * stream
        squares = (squares[:, 0:128] + squares[:, 128:256]) + (
            squares[:, 256:384] + squares[:, 384:512]
        )
        put(a0, l, 0, 0, 5, squares)
        scaled = (stream * gain_s[l : l + 1, :].astype(jnp.float32)).astype(jnp.bfloat16)
        weights[l][0].wait()
        part = jnp.dot(scaled, wq_s[l, :, 0:640], preferred_element_type=jnp.float32)
        for t in range(5):
            put(a0, l, 0, 0, t, part[:, t * 128 : (t + 1) * 128])
        if l == 0:
            pl.semaphore_wait(barrier, 6 + NTP - 1)
        a0_1 = exchange(a0, l, 0, "x", a_send.at[0], a_recv.at[0])
        weights[l][1].wait()
        weights[l][2].wait()
        part = jnp.dot(scaled, wq_s[l, :, 640:1024], preferred_element_type=jnp.float32)
        key_part = jnp.dot(scaled, wk_s[l], preferred_element_type=jnp.float32)
        value_part = jnp.dot(scaled, wv_s[l], preferred_element_type=jnp.float32)
        for t in range(3):
            put(a1, l, 0, 0, t, part[:, t * 128 : (t + 1) * 128])
        put(a1, l, 0, 0, 3, key_part)
        put(a1, l, 0, 0, 4, value_part)
        a1_1 = exchange(a1, l, 0, "y", a_send.at[1], a_recv.at[1])
        arrive(a0_1)
        for t in range(T0):
            put(a0, l, 1, 0, t, summed(a0, l, 0, t))
        a0_2 = exchange(a0, l, 1, "y", a_send.at[0], a_recv.at[0])
        arrive(a1_1)
        for t in range(T1):
            put(a1, l, 1, 0, t, summed(a1, l, 0, t))
        a1_2 = exchange(a1, l, 1, "x", a_send.at[1], a_recv.at[1])

        weights[l][3].wait()
        weights[l][4].wait()
        arrive(a0_2)
        total = jnp.sum(summed(a0, l, 1, 5), axis=1, keepdims=True)
        inverse = lax.rsqrt(total / D + norm_eps)
        cos_l = cosine * inverse
        sin_l = sine * inverse

        def turn(u):
            return u * cos_l + pltpu.roll(u, HD // 2, 1) * sin_l

        heads = [turn(summed(a0, l, 1, t)) for t in range(5)]
        arrive(a1_2)
        heads += [turn(summed(a1, l, 1, t)) for t in range(3)]
        new_key = turn(summed(a1, l, 1, 3)).astype(jnp.bfloat16).astype(jnp.float32)
        new_value = (summed(a1, l, 1, 4) * inverse).astype(jnp.bfloat16).astype(jnp.float32)
        query = jnp.concatenate(heads, axis=0).astype(jnp.bfloat16)

        score = None
        for b in range(0, BATCH, 2):
            keys = kc_s[l, b : b + 2, 0].reshape(2 * POS, HD)
            both = lax.dot_general(
                query, keys, (((1,), (1,)), ((), ())), preferred_element_type=jnp.float32
            )
            first, second = both[:, :POS], both[:, POS:]
            score = first if score is None else jnp.where(row_seq == b, first, score)
            score = jnp.where(row_seq == b + 1, second, score)
        masked = jnp.where(usable, score * logit_multiplier, mask_fill)
        local_max = jnp.max(masked, axis=1, keepdims=True)
        weight = jnp.where(usable, jnp.exp(masked - local_max), 0.0)
        local_sum = jnp.sum(weight, axis=1, keepdims=True)
        rounded = weight.astype(jnp.bfloat16).astype(jnp.float32)
        wide = jnp.concatenate(
            [jnp.where(row_seq == b, rounded, 0.0).astype(jnp.bfloat16) for b in range(BATCH)],
            axis=1,
        )
        values = vc_s[l, :, 0].reshape(BATCH * POS, HD)
        local_out = jnp.dot(wide, values, preferred_element_type=jnp.float32)

        sends = []
        for half, buf in enumerate((b0, b1)):
            stats = jnp.zeros((BATCH, HD), jnp.float32)
            for j in range(4):
                h = half * 4 + j
                rows = slice(h * 8, h * 8 + 8)
                put(buf, l, 0, 0, j, local_out[rows])
                stats = jnp.where(lane == j, local_max[rows], stats)
                stats = jnp.where(lane == 4 + j, local_sum[rows], stats)
            put(buf, l, 0, 0, 4, stats)
            sends.append(
                exchange(buf, l, 0, "xy"[half], b_send.at[half], b_recv.at[half])
            )

        own = [jnp.zeros((BATCH, HD), jnp.float32)] * 2
        for h in range(HEADS):
            rounded_head = heads[h].astype(jnp.bfloat16).astype(jnp.float32)
            dots = jnp.sum(rounded_head * new_key, axis=1, keepdims=True) * logit_multiplier
            own[h // 4] = jnp.where(lane == h % 4, dots, own[h // 4])

        def factors(buf, stage):
            stats = [tile(buf, l, stage, s, 4) for s in range(4)]
            top = jnp.maximum(
                jnp.maximum(stats[0], stats[1]), jnp.maximum(stats[2], stats[3])
            )
            scale = [jnp.exp(s - top) for s in stats]
            sums = [s * pltpu.roll(f, 4, 1) for s, f in zip(stats, scale)]
            return top, scale, (sums[0] + sums[1]) + (sums[2] + sums[3])

        second = []
        for half, buf in enumerate((b0, b1)):
            arrive(sends[half])
            top, scale, sums = factors(buf, 0)
            for j in range(4):
                merged = [tile(buf, l, 0, s, j) * spread(scale[s], j) for s in range(4)]
                put(buf, l, 1, 0, j, (merged[0] + merged[1]) + (merged[2] + merged[3]))
            put(buf, l, 1, 0, 4, jnp.where(lane < 4, top, jnp.where(lane < 8, sums, 0.0)))
            second.append(
                exchange(buf, l, 1, "yx"[half], b_send.at[half], b_recv.at[half])
            )

        weights[l][5].wait()
        contribution = None
        for half, buf in enumerate((b0, b1)):
            arrive(second[half])
            top, scale, sums = factors(buf, 1)
            row_top = jnp.maximum(top, own[half])
            carried = jnp.exp(top - row_top)
            fresh = jnp.exp(own[half] - row_top)
            denominator = pltpu.roll(sums, HD - 4, 1) * carried + fresh
            denominator = jnp.where(lane < 4, denominator, 1.0)
            carried = carried / denominator
            fresh = fresh.astype(jnp.bfloat16).astype(jnp.float32) / denominator
            scale = [s * carried for s in scale]
            context = []
            for j in range(4):
                merged = [tile(buf, l, 1, s, j) * spread(scale[s], j) for s in range(4)]
                context.append(
                    (merged[0] + merged[1])
                    + (merged[2] + merged[3])
                    + spread(fresh, j) * new_value
                )
            context = jnp.concatenate(context, axis=1).astype(jnp.bfloat16)
            term = jnp.dot(
                context,
                wo_s[l, half * 512 : (half + 1) * 512, :],
                preferred_element_type=jnp.float32,
            )
            contribution = term if contribution is None else contribution + term
        cbuf[l, pl.ds(tp, 1)] = jnp.concatenate(
            [contribution[:, t * 128 : (t + 1) * 128] for t in range(4)], axis=0
        )[None]
        copies = []
        for k in (4, 5, 3, 2, 6, 1, 7):
            c = pltpu.make_async_remote_copy(
                src_ref=cbuf.at[l, tp],
                dst_ref=cbuf.at[l, tp],
                send_sem=c_send.at[l, k],
                recv_sem=c_recv.at[l, k],
                device_id={"tp": (tp + k) % NTP},
            )
            c.start()
            copies.append(c)
        pending.extend(copies)
        arrive(copies)
        tiles = []
        for t in range(4):
            terms = [cbuf[l, s, pl.ds(t * 8, 8), :] for s in range(NTP)]
            tiles.append(
                ((terms[0] + terms[1]) + (terms[2] + terms[3]))
                + ((terms[4] + terms[5]) + (terms[6] + terms[7]))
            )
        stream = stream + jnp.concatenate(tiles, axis=1)

    out[...] = stream
    for c in pending:
        c.wait_send()


def on_device(*args):
    hbm = pl.BlockSpec(memory_space=pl.ANY)
    f32, bf16 = jnp.float32, jnp.bfloat16
    dma = pltpu.SemaphoreType.DMA
    return pl.pallas_call(
        kernel,
        out_shape=jax.ShapeDtypeStruct((BATCH, FEATS), f32),
        in_specs=[hbm] * 9,
        out_specs=pl.BlockSpec(memory_space=pltpu.VMEM),
        scratch_shapes=[
            pltpu.VMEM((BATCH, FEATS), bf16),
            pltpu.VMEM((LAYERS, FEATS), bf16),
            pltpu.SMEM((BATCH,), jnp.int32),
            pltpu.VMEM((LAYERS, FEATS, HEADS * HD), bf16),
            pltpu.VMEM((LAYERS, FEATS, HD), bf16),
            pltpu.VMEM((LAYERS, FEATS, HD), bf16),
            pltpu.VMEM((LAYERS, HEADS * HD, FEATS), bf16),
            pltpu.VMEM((LAYERS, BATCH, 1, POS, HD), bf16),
            pltpu.VMEM((LAYERS, BATCH, 1, POS, HD), bf16),
            pltpu.VMEM((LAYERS, 2, NX, T0 * 8, HD), f32),
            pltpu.VMEM((LAYERS, 2, NX, T1 * 8, HD), f32),
            pltpu.VMEM((LAYERS, 2, NX, TB * 8, HD), f32),
            pltpu.VMEM((LAYERS, 2, NX, TB * 8, HD), f32),
            pltpu.VMEM((LAYERS, NTP, 4 * 8, HD), f32),
            dma((3,)),
            dma((LAYERS, 6)),
            dma((2, LAYERS, 2, NX)),
            dma((2, LAYERS, 2, NX)),
            dma((2, LAYERS, 2, NX)),
            dma((2, LAYERS, 2, NX)),
            dma((LAYERS, NTP)),
            dma((LAYERS, NTP)),
        ],
        compiler_params=pltpu.CompilerParams(collective_id=0, has_side_effects=True),
    )(*args)


def solution(mesh):
    return jax.shard_map(
        on_device,
        mesh=mesh,
        in_specs=(
            P(None, "ctx"),
            P(None, "ctx"),
            P(None, "ctx", "tp"),
            P(None, "ctx", "tp"),
            P(None, "ctx", "tp"),
            P(None, "tp", "ctx"),
            P(None, None, "tp", "ctx", None),
            P(None, None, "tp", "ctx", None),
            P(),
        ),
        out_specs=P(None, "ctx"),
        check_vma=False,
    )
```
